32 devices in a mesh: shard: 8 (over y, x, core), dp: 4 (over z).
Axes of the slice: x: 2, y: 2, z: 4, core: 2. Of those that a mesh axis runs over, the one named last changes fastest.
Arguments:
- grad: float32 [288, 128, 4096], P('shard', 'dp'), may hold values from -252 to 252
- param: bfloat16 [288, 128, 4096], P('shard', 'dp'), may hold values from -0.119628906 to 0.119628906
- row_state: float32 [288, 128], P('shard', 'dp'), may hold values from 0.3 to 27
- col_state: float32 [3, 4096], replicated, may hold values from 0.002 to 400
- block_start: int32 [8], replicated, may hold values from 0 to 143, as said below
- block_matrix: int32 [144], replicated, may hold values from 0 to 2, as said below
- step: int32 [1], replicated, may hold values from 2 to 11
Outputs:
- new_params: bfloat16 [18432, 4096], P(None, 'shard')
- new_row_state: float32 [288, 128], P('shard', 'dp')
- new_col_state: float32 [3, 4096], replicated
The draws below stay inside these ranges and needn't reach their ends.
Inputs may be any that keep to these rules, and one draw needn't show every extreme that they name: block_start rises from 0 at index 0; every shard index owns between 1 and 36 consecutive global blocks, held in its first slots, and some index owns exactly 36; slots past a device's owned count hold values that no output reads. `block_matrix`: ids 0 and 1 each label 4096 / 128 blocks and id 2 labels 10240 / 128 blocks, in any order.
All inputs are finite; a program needn't handle non-finite values.
Results may differ from the reference program's by a relative error of at most 0.0004.
Values may be sent and summed in bfloat16 or wider, within the bound.
A program may use at most 192 MiB of HBM per device.

```python
import math
import jax
import jax.numpy as jnp
from jax import lax

D = 4096
FF = 10240
BLOCK = 128
MATS = 3
NB = 144
CAP = 36
N_SHARD = 8


def draw_grad(key, part):
    noise_key, row_key, col_key = jax.random.split(jax.random.fold_in(key, 11), 3)
    slot_total = N_SHARD * CAP
    draw_base = jnp.clip(jax.random.normal(noise_key, (slot_total, BLOCK, D), jnp.float32), -4.0, 4.0)
    row_scale = jnp.exp(jax.random.uniform(row_key, (slot_total, BLOCK), jnp.float32, math.log(0.3), math.log(3.0)))
    col_scale = jnp.exp(jax.random.uniform(col_key, (D,), jnp.float32, math.log(0.3), math.log(3.0)))
    position = jnp.arange(slot_total, dtype=jnp.float32) / max(slot_total - 1, 1)
    ramp_scale = 1.0 + 2.0 * position
    return draw_base * (row_scale * ramp_scale[:, None])[:, :, None] * col_scale[None, None, :]


def draw_row_state(key, part):
    slot_total = N_SHARD * CAP
    state_key = jax.random.fold_in(key, 23)
    position = jnp.arange(slot_total, dtype=jnp.float32) / max(slot_total - 1, 1)
    values = jnp.exp(jax.random.uniform(state_key, (slot_total, BLOCK), jnp.float32, math.log(0.3), math.log(3.0)))
    ramp_scale = 1.0 + 2.0 * position
    return values * ramp_scale[:, None]


def draw_col_state(key, part):
    state_key = jax.random.fold_in(key, 37)
    lowest = jnp.array([0.002, 64.0, 0.002], jnp.float32)
    factor = jnp.exp(jax.random.uniform(state_key, (MATS, D), jnp.float32, 0.0, math.log(4.0)))
    return lowest[:, None] * factor


def draw_block_matrix(key, part):
    order_key = jax.random.fold_in(key, 41)
    block_index = jnp.arange(NB, dtype=jnp.int32)
    first_end = D // BLOCK
    second_end = 2 * (D // BLOCK)
    labels = (block_index >= first_end).astype(jnp.int32) + (block_index >= second_end).astype(jnp.int32)
    return jax.random.permutation(order_key, labels).astype(jnp.int32)


def draw_block_start(key, part):
    busy_key, move_key = jax.random.split(jax.random.fold_in(key, 53))
    busy_device = jax.random.randint(busy_key, (), 0, N_SHARD - 1)
    last_device = N_SHARD - 1
    rest_blocks = NB - CAP - 1
    base_count = rest_blocks // (N_SHARD - 2)
    extra_count = rest_blocks % (N_SHARD - 2)
    device_ids = jnp.arange(N_SHARD, dtype=jnp.int32)
    position_rank = device_ids - (device_ids > busy_device).astype(jnp.int32)
    spread_count = base_count + (position_rank < extra_count).astype(jnp.int32)
    counts = jnp.where(device_ids == busy_device, CAP, jnp.where(device_ids == last_device, 1, spread_count)).astype(jnp.int32)

    def move(turn, counts):
        turn_key = jax.random.fold_in(move_key, turn)
        pair_key, amount_key = jax.random.split(turn_key)
        ends_pair = jax.random.randint(pair_key, (2,), 0, N_SHARD)
        source = ends_pair[0]
        target = ends_pair[1]
        wanted = jax.random.randint(amount_key, (), 0, CAP)
        usable = (source != busy_device) & (target != busy_device) & (source != target) & (source != last_device) & (target != last_device)
        amount = jnp.minimum(jnp.minimum(wanted, counts[source] - 1), CAP - counts[target])
        amount = jnp.where(usable, jnp.maximum(amount, 0), 0).astype(jnp.int32)
        return counts.at[source].add(-amount).at[target].add(amount)
    counts = lax.fori_loop(0, 4 * N_SHARD, move, counts)
    return (jnp.cumsum(counts) - counts).astype(jnp.int32)


def levels(stream_key, dims, pieces, least, largest):
    gain = 1.0
    for axis_at, parts in pieces:
        draws = jax.random.uniform(jax.random.fold_in(jax.random.fold_in(stream_key, 6), axis_at), (parts,), jnp.float32, least / len(pieces), largest / len(pieces))
        gain = gain * jnp.repeat(jnp.exp(draws), dims[axis_at] // parts).reshape((-1,) + (1,) * (len(dims) - 1 - axis_at))
    return gain


def normal_values(stream_key, shape, width, limit, shards=(), kind=jnp.bfloat16):
    values = width * jax.random.normal(stream_key, shape, jnp.float32)
    if shards:
        values = values * levels(stream_key, shape, shards, -0.22, 0.18)
    return jnp.clip(values, -limit, limit).astype(kind)


def setup_inputs(seed: int = 0) -> dict:
    streams_of = jax.random.split(jax.random.key(seed), 8)
    return {
        "grad": draw_grad(jax.random.fold_in(streams_of[7], 71), 0),
        "param": normal_values(streams_of[1], (N_SHARD * CAP, BLOCK, D), 0.02, 0.119628906, ((0, 8), (1, 4))),
        "row_state": draw_row_state(jax.random.fold_in(streams_of[7], 71), 0),
        "col_state": draw_col_state(jax.random.fold_in(streams_of[7], 71), 0),
        "block_start": draw_block_start(jax.random.fold_in(streams_of[7], 71), 0),
        "block_matrix": draw_block_matrix(jax.random.fold_in(streams_of[7], 71), 0),
        "step": jax.random.randint(streams_of[6], (1,), 2, 12).astype(jnp.int32),
    }


def scale_grad(grad, safe_rows, matrix_pick, new_cols, row_avg):
    slot_cols = jnp.dot(matrix_pick, new_cols, precision=lax.Precision.HIGHEST)
    slot_avg = jnp.dot(matrix_pick, row_avg, precision=lax.Precision.HIGHEST)
    return grad / jnp.sqrt(safe_rows[:, :, None] * slot_cols[:, None, :] / slot_avg[:, None, None])

def reference(grad, param, row_state, col_state, block_start, block_matrix, step):
    slot_total = grad.shape[0]
    block_ends = jnp.concatenate([block_start[1:], jnp.full((1,), NB, jnp.int32)])
    slot_ids = jnp.arange(slot_total, dtype=jnp.int32)
    owner_shard = slot_ids // CAP
    within = slot_ids % CAP
    owned_count = (block_ends - block_start)[owner_shard]
    live_slot = within < owned_count
    block_ids = jnp.minimum(block_start[owner_shard] + within, NB - 1).astype(jnp.int32)
    matrix_ids = jnp.where(live_slot, block_matrix[block_ids], 0)
    matrix_pick = (matrix_ids[:, None] == jnp.arange(3, dtype=jnp.int32)[None, :]).astype(jnp.float32)
    member = matrix_pick * live_slot[:, None].astype(jnp.float32)
    row_count = jnp.array([D, D, FF], jnp.float32)
    step_value = step[0].astype(jnp.float32)
    decay_rate = 1.0 - step_value ** (-0.8)
    learn_rate = 1.0 / jnp.sqrt(jnp.maximum(step_value, 10000.0))
    squares = grad * grad
    new_rows = jnp.where(live_slot[:, None], decay_rate * row_state + (1.0 - decay_rate) * lax.optimization_barrier(jnp.sum(squares, axis=2)) / D, 0.0)
    safe_rows = jnp.where(live_slot[:, None], new_rows, 1.0)
    col_total = jnp.einsum('sm,sd->md', member, lax.optimization_barrier(jnp.sum(squares, axis=1)), precision=lax.Precision.HIGHEST)
    new_cols = decay_rate * col_state + (1.0 - decay_rate) * col_total / row_count[:, None]
    row_avg = jnp.dot(lax.optimization_barrier(jnp.sum(new_rows, axis=1)), member, precision=lax.Precision.HIGHEST) / row_count
    scaled = scale_grad(grad, safe_rows, matrix_pick, new_cols, row_avg)
    square_total = jnp.dot(lax.optimization_barrier(jnp.sum(scaled * scaled, axis=(1, 2))), member, precision=lax.Precision.HIGHEST)
    clip_factor = jnp.maximum(1.0, jnp.sqrt(square_total / (row_count * D)))
    slot_clip = jnp.dot(matrix_pick, clip_factor, precision=lax.Precision.HIGHEST)
    updated = jnp.where(live_slot[:, None, None], param.astype(jnp.float32) - learn_rate * scaled / slot_clip[:, None, None], 0.0).astype(jnp.bfloat16)
    block_index = jnp.arange(NB, dtype=jnp.int32)
    block_owner = lax.optimization_barrier(jnp.sum((block_start[None, :] <= block_index[:, None]).astype(jnp.int32), axis=1)) - 1
    slot_of = (block_owner * CAP + block_index - jnp.take(block_start, block_owner)).astype(jnp.int32)
    new_params = jnp.take(updated, slot_of, axis=0).reshape(NB * BLOCK, D)
    return (new_params, new_rows, new_cols)
```

```python
import functools

import jax
import jax.numpy as jnp
from jax import lax
from jax.experimental import pallas as pl
from jax.experimental.pallas import tpu as pltpu
from jax.sharding import PartitionSpec as P

D = 4096
FF = 10240
MATS = 3
CHUNK = 8


def slots_per_step(slot_count):
    return max(n for n in range(1, 5) if slot_count % n == 0)


def sums_kernel(group, mats, ints_ref, floats_ref, grad_ref, state_ref, rows_ref, sums_ref, cols_acc, weighted_acc, rows_acc):
    step = pl.program_id(0)
    owned = ints_ref[0]
    beta = floats_ref[0]
    gain = floats_ref[1]
    height, width = grad_ref.shape[1], grad_ref.shape[2]

    @pl.when(step == 0)
    def _():
        cols_acc[...] = jnp.zeros_like(cols_acc)
        weighted_acc[...] = jnp.zeros_like(weighted_acc)
        rows_acc[...] = jnp.zeros_like(rows_acc)

    for j in range(group):
        slot = step * group + j

        @pl.when(slot >= owned)
        def _():
            rows_ref[j] = jnp.zeros_like(rows_ref[j])

        @pl.when(slot < owned)
        def _():
            m = ints_ref[2 + slot]
            squares = grad_ref[j] * grad_ref[j]
            rows = beta * state_ref[j] + gain * jnp.sum(squares, axis=1, keepdims=True)
            rows_ref[j] = rows
            tall = (height // 8, 8, width)
            cols_acc[m] += jnp.sum(squares.reshape(tall), axis=0)
            weighted_acc[m] += jnp.sum((squares * (1.0 / rows)).reshape(tall), axis=0)
            rows_acc[m] += jnp.sum(jnp.broadcast_to(rows, (height, 128)).reshape(height // 8, 8, 128), axis=0)

    @pl.when(step == pl.num_programs(0) - 1)
    def _():
        sums_ref[...] = jnp.zeros_like(sums_ref)
        for m in range(mats):
            sums_ref[m : m + 1, :] = jnp.sum(cols_acc[m], axis=0, keepdims=True)
            sums_ref[mats + m : mats + m + 1, :] = jnp.sum(weighted_acc[m], axis=0, keepdims=True)
            sums_ref[2 * mats : 2 * mats + 1, m * 128 : m * 128 + 128] = jnp.sum(rows_acc[m], axis=0, keepdims=True)


def update_kernel(group, mats, parts, row_counts, ints_ref, floats_ref, grad_ref, param_ref, rows_ref, total_ref, state_ref, *refs):
    chunk_refs, (cols_ref, factor) = refs[:-2], refs[-2:]
    step = pl.program_id(0)
    owned, last = ints_ref[0], ints_ref[1]
    beta, rest, rate = floats_ref[0], floats_ref[2], floats_ref[3]
    height, width = grad_ref.shape[1], grad_ref.shape[2]
    cut = width // parts

    @pl.when(step == 0)
    def _():
        for m in range(mats):
            count = row_counts[m]
            cols = beta * state_ref[m : m + 1, :] + rest * (total_ref[m : m + 1, :] / count)
            cols_ref[m : m + 1, :] = cols
            average = total_ref[2 * mats : 2 * mats + 1, m * 128 : m * 128 + 1] / count
            weighted = total_ref[mats + m : mats + m + 1, :]
            square = average * jnp.sum(weighted / cols, axis=1, keepdims=True)
            clip = jnp.maximum(1.0, jnp.sqrt(square / (count * width)))
            factor[m] = lax.rsqrt(cols) * (jnp.sqrt(average) * rate / clip)

    @pl.when(step <= last)
    def _():
        for j in range(group):
            slot = step * group + j

            @pl.when(slot < owned)
            def _():
                m = ints_ref[2 + slot]
                scale = lax.rsqrt(rows_ref[j])
                for k, chunk_ref in enumerate(chunk_refs):
                    at = slice(k * CHUNK, (k + 1) * CHUNK)
                    for n in range(parts):
                        span = slice(n * cut, (n + 1) * cut)
                        new = param_ref[j, at, span].astype(jnp.float32) - grad_ref[j, at, span] * scale[at] * factor[m, :, span]
                        chunk_ref[n, j] = new.astype(chunk_ref.dtype)


def pick_kernel(slot_ref, in_ref, out_ref):
    def move(b, carry):
        out_ref[b] = in_ref[slot_ref[b]]
        return carry

    lax.fori_loop(0, out_ref.shape[0], move, 0, unroll=8)


def place_kernel(in_ref, *refs):
    refs[-1][:, :, 0] = in_ref[...]


def body(parts, grad, param, row_state, col_state, block_start, block_matrix, step):
    slot_count, height, width = grad.shape
    mats = col_state.shape[0]
    total_blocks = block_matrix.shape[0]
    group = slots_per_step(slot_count)
    steps = slot_count // group
    chunks = height // CHUNK
    cut = width // parts
    row_counts = (float(D), float(D), float(FF))

    shard_index = lax.axis_index("shard")
    block_ends = jnp.concatenate([block_start[1:], jnp.full((1,), total_blocks, jnp.int32)])
    at_shard = jnp.arange(parts, dtype=jnp.int32) == shard_index
    first_block = jnp.sum(jnp.where(at_shard, block_start, 0))
    owned = jnp.sum(jnp.where(at_shard, block_ends - block_start, 0))
    block_index = jnp.arange(total_blocks, dtype=jnp.int32)
    slot_blocks = first_block + jnp.arange(slot_count, dtype=jnp.int32)
    matrix_ids = jnp.sum(
        jnp.where(slot_blocks[:, None] == block_index[None, :], block_matrix[None, :], 0), axis=1
    )
    started = block_start[None, :] <= block_index[:, None]
    owner = jnp.sum(started.astype(jnp.int32), axis=1) - 1
    owner_start = jnp.max(jnp.where(started, block_start[None, :], 0), axis=1)
    slot_of = owner * slot_count + block_index - owner_start
    ints = jnp.concatenate([jnp.stack([owned, (owned - 1) // group]), matrix_ids]).astype(jnp.int32)
    step_value = step[0].astype(jnp.float32)
    beta = 1.0 - step_value ** (-0.8)
    rate = 1.0 / jnp.sqrt(jnp.maximum(step_value, 10000.0))
    floats = jnp.stack([beta, (1.0 - beta) / width, 1.0 - beta, rate])

    smem = pl.BlockSpec(memory_space=pltpu.SMEM)

    def live(i, ints_ref):
        return jnp.minimum(i, ints_ref[1])

    new_rows, sums = pl.pallas_call(
        functools.partial(sums_kernel, group, mats),
        grid_spec=pltpu.PrefetchScalarGridSpec(
            num_scalar_prefetch=1,
            grid=(steps,),
            in_specs=[
                smem,
                pl.BlockSpec((group, height, width), lambda i, s: (live(i, s), 0, 0)),
                pl.BlockSpec((group, height, 1), lambda i, s: (i, 0, 0)),
            ],
            out_specs=[
                pl.BlockSpec((group, height, 1), lambda i, s: (i, 0, 0)),
                pl.BlockSpec((8, width), lambda i, s: (0, 0)),
            ],
            scratch_shapes=[
                pltpu.VMEM((mats, 8, width), jnp.float32),
                pltpu.VMEM((mats, 8, width), jnp.float32),
                pltpu.VMEM((mats, 8, 128), jnp.float32),
            ],
        ),
        out_shape=[
            jax.ShapeDtypeStruct((slot_count, height, 1), jnp.float32),
            jax.ShapeDtypeStruct((8, width), jnp.float32),
        ],
        compiler_params=pltpu.CompilerParams(vmem_limit_bytes=60 * 2**20),
        cost_estimate=pl.CostEstimate(flops=grad.size * 6, bytes_accessed=grad.size * 4, transcendentals=0),
        name="sums",
    )(ints, floats, grad, row_state[:, :, None])

    total = lax.psum(sums, ("shard", "dp"))

    outs = pl.pallas_call(
        functools.partial(update_kernel, group, mats, parts, row_counts),
        grid_spec=pltpu.PrefetchScalarGridSpec(
            num_scalar_prefetch=1,
            grid=(steps,),
            in_specs=[
                smem,
                pl.BlockSpec((group, height, width), lambda i, s: (live(i, s), 0, 0)),
                pl.BlockSpec((group, height, width), lambda i, s: (live(i, s), 0, 0)),
                pl.BlockSpec((group, height, 1), lambda i, s: (live(i, s), 0, 0)),
                pl.BlockSpec((8, width), lambda i, s: (0, 0)),
                pl.BlockSpec((mats, width), lambda i, s: (0, 0)),
            ],
            out_specs=[
                pl.BlockSpec((parts, group, CHUNK, cut), lambda i, s: (0, live(i, s), 0, 0))
                for _ in range(chunks)
            ]
            + [pl.BlockSpec((mats, width), lambda i, s: (0, 0))],
            scratch_shapes=[pltpu.VMEM((mats, 1, width), jnp.float32)],
        ),
        out_shape=[
            jax.ShapeDtypeStruct((parts, slot_count, CHUNK, cut), jnp.bfloat16) for _ in range(chunks)
        ]
        + [jax.ShapeDtypeStruct((mats, width), jnp.float32)],
        compiler_params=pltpu.CompilerParams(vmem_limit_bytes=60 * 2**20),
        cost_estimate=pl.CostEstimate(flops=grad.size * 6, bytes_accessed=grad.size * 8, transcendentals=0),
        name="update",
    )(ints, floats, grad, param, new_rows, total, col_state)
    new_cols = outs[-1]

    dp = lax.axis_size("dp")
    piece_bytes = total_blocks * CHUNK * cut * 2
    placed = None
    run = 12 if total_blocks % 12 == 0 else 1
    for k in range(chunks):
        moved = lax.all_to_all(outs[k], "shard", split_axis=0, concat_axis=0, tiled=True)
        picked = pl.pallas_call(
            pick_kernel,
            in_specs=[smem, pl.BlockSpec(memory_space=pltpu.VMEM)],
            out_specs=pl.BlockSpec(memory_space=pltpu.VMEM),
            out_shape=jax.ShapeDtypeStruct((total_blocks, CHUNK, cut), jnp.bfloat16),
            compiler_params=pltpu.CompilerParams(vmem_limit_bytes=16 * 2**20),
            cost_estimate=pl.CostEstimate(flops=0, bytes_accessed=3 * piece_bytes, transcendentals=0),
            name="pick",
        )(slot_of, moved.reshape(parts * slot_count, CHUNK, cut))
        spread = lax.all_gather(picked, "dp", axis=1, tiled=True)
        spread = spread.reshape(total_blocks, dp, CHUNK, cut)
        old = [] if placed is None else [placed]
        placed = pl.pallas_call(
            place_kernel,
            grid=(total_blocks // run,),
            in_specs=[pl.BlockSpec((run, dp, CHUNK, cut), lambda i: (i, 0, 0, 0))]
            + [pl.BlockSpec(memory_space=pl.ANY) for _ in old],
            out_specs=pl.BlockSpec((run, dp, 1, CHUNK, cut), functools.partial(lambda k, i: (i, 0, k, 0, 0), k)),
            out_shape=jax.ShapeDtypeStruct((total_blocks, dp, chunks, CHUNK, cut), jnp.bfloat16),
            input_output_aliases={1: 0} if old else {},
            compiler_params=pltpu.CompilerParams(vmem_limit_bytes=60 * 2**20),
            cost_estimate=pl.CostEstimate(flops=0, bytes_accessed=2 * dp * piece_bytes, transcendentals=0),
            name="place",
        )(spread, *old)
    new_params = placed.reshape(total_blocks * dp * height, cut)
    return new_params, new_rows[:, :, 0], new_cols


def solution(mesh):
    return jax.shard_map(
        functools.partial(body, mesh.shape["shard"]),
        mesh=mesh,
        in_specs=(
            P("shard", "dp", None),
            P("shard", "dp", None),
            P("shard", "dp"),
            P(),
            P(),
            P(),
            P(),
        ),
        out_specs=(P(None, "shard"), P("shard", "dp"), P()),
        check_vma=False,
    )
```

```python
import functools

import jax
import jax.numpy as jnp
from jax import lax
from jax.experimental import pallas as pl
from jax.experimental.pallas import tpu as pltpu
from jax.sharding import PartitionSpec as P

D = 4096
FF = 10240
MATS = 3
CHUNK = 8


def slots_per_step(slot_count):
    return max(n for n in range(1, 5) if slot_count % n == 0)


def sums_kernel(group, mats, piece, ints_ref, floats_ref, grad_ref, state_ref, rows_ref, sums_ref, cols_acc, weighted_acc, rows_acc):
    step = pl.program_id(0)
    owned = ints_ref[0]
    beta = floats_ref[0]
    gain = floats_ref[1]
    height, width = grad_ref.shape[1], grad_ref.shape[2]

    @pl.when(step == 0)
    def _():
        cols_acc[...] = jnp.zeros_like(cols_acc)
        weighted_acc[...] = jnp.zeros_like(weighted_acc)
        rows_acc[...] = jnp.zeros_like(rows_acc)

    for j in range(group):
        slot = step * group + j

        @pl.when(slot >= owned)
        def _():
            rows_ref[j] = jnp.zeros_like(rows_ref[j])

        @pl.when(slot < owned)
        def _():
            m = ints_ref[2 + slot]
            squares = grad_ref[j] * grad_ref[j]
            rows = beta * state_ref[j] + gain * jnp.sum(squares, axis=1, keepdims=True)
            rows_ref[j] = rows
            tall = (height // 8, 8, width)
            cols_acc[m] += jnp.sum(squares.reshape(tall), axis=0)
            weighted_acc[m] += jnp.sum((squares * (1.0 / rows)).reshape(tall), axis=0)
            rows_acc[m] += jnp.sum(jnp.broadcast_to(rows, (height, 128)).reshape(height // 8, 8, 128), axis=0)

    @pl.when(step == pl.num_programs(0) - 1)
    def _():
        sums_ref[...] = jnp.zeros_like(sums_ref)
        for m in range(mats):
            sums_ref[m : m + 1, :] = jnp.sum(cols_acc[m], axis=0, keepdims=True)
            sums_ref[mats + m : mats + m + 1, :] = jnp.sum(weighted_acc[m], axis=0, keepdims=True)
            spot = lax.broadcasted_iota(jnp.int32, (1, sums_ref.shape[1]), 1) % piece == m
            part = jnp.sum(rows_acc[m], axis=0, keepdims=True)[:, 0:1]
            sums_ref[2 * mats : 2 * mats + 1, :] += jnp.where(spot, part, 0.0)


def update_kernel(group, mats, parts, row_counts, ints_ref, floats_ref, grad_ref, param_ref, rows_ref, total_ref, state_ref, *refs):
    chunk_refs, (cols_ref, factor) = refs[:-2], refs[-2:]
    step = pl.program_id(0)
    owned, last = ints_ref[0], ints_ref[1]
    beta, rest, rate = floats_ref[0], floats_ref[2], floats_ref[3]
    height, width = grad_ref.shape[1], grad_ref.shape[2]
    cut = width // parts

    @pl.when(step == 0)
    def _():
        for m in range(mats):
            count = row_counts[m]
            cols = beta * state_ref[m : m + 1, :] + rest * (total_ref[m : m + 1, :] / count)
            cols_ref[m : m + 1, :] = cols
            average = total_ref[2 * mats : 2 * mats + 1, m : m + 1] / count
            weighted = total_ref[mats + m : mats + m + 1, :]
            square = average * jnp.sum(weighted / cols, axis=1, keepdims=True)
            clip = jnp.maximum(1.0, jnp.sqrt(square / (count * width)))
            factor[m] = lax.rsqrt(cols) * (jnp.sqrt(average) * rate / clip)

    @pl.when(step <= last)
    def _():
        for j in range(group):
            slot = step * group + j

            @pl.when(slot < owned)
            def _():
                m = ints_ref[2 + slot]
                scale = lax.rsqrt(rows_ref[j])
                for k, chunk_ref in enumerate(chunk_refs):
                    at = slice(k * CHUNK, (k + 1) * CHUNK)
                    for n in range(parts):
                        span = slice(n * cut, (n + 1) * cut)
                        new = param_ref[j, at, span].astype(jnp.float32) - grad_ref[j, at, span] * scale[at] * factor[m, :, span]
                        chunk_ref[n, j] = new.astype(chunk_ref.dtype)


def pick_kernel(slot_ref, in_ref, out_ref):
    def move(b, carry):
        out_ref[b] = in_ref[slot_ref[b]]
        return carry

    lax.fori_loop(0, out_ref.shape[0], move, 0, unroll=8)


def place_kernel(in_ref, *refs):
    refs[-1][:, :, 0] = in_ref[...]


def body(parts, grad, param, row_state, col_state, block_start, block_matrix, step):
    slot_count, height, width = grad.shape
    mats = col_state.shape[0]
    total_blocks = block_matrix.shape[0]
    group = slots_per_step(slot_count)
    steps = slot_count // group
    chunks = height // CHUNK
    cut = width // parts
    every = lax.axis_size(("shard", "dp"))
    piece = width // every
    row_counts = (float(D), float(D), float(FF))

    shard_index = lax.axis_index("shard")
    block_ends = jnp.concatenate([block_start[1:], jnp.full((1,), total_blocks, jnp.int32)])
    at_shard = jnp.arange(parts, dtype=jnp.int32) == shard_index
    first_block = jnp.sum(jnp.where(at_shard, block_start, 0))
    owned = jnp.sum(jnp.where(at_shard, block_ends - block_start, 0))
    block_index = jnp.arange(total_blocks, dtype=jnp.int32)
    slot_blocks = first_block + jnp.arange(slot_count, dtype=jnp.int32)
    matrix_ids = jnp.sum(
        jnp.where(slot_blocks[:, None] == block_index[None, :], block_matrix[None, :], 0), axis=1
    )
    started = block_start[None, :] <= block_index[:, None]
    owner = jnp.sum(started.astype(jnp.int32), axis=1) - 1
    owner_start = jnp.max(jnp.where(started, block_start[None, :], 0), axis=1)
    slot_of = owner * slot_count + block_index - owner_start
    ints = jnp.concatenate([jnp.stack([owned, (owned - 1) // group]), matrix_ids]).astype(jnp.int32)
    step_value = step[0].astype(jnp.float32)
    beta = 1.0 - step_value ** (-0.8)
    rate = 1.0 / jnp.sqrt(jnp.maximum(step_value, 10000.0))
    floats = jnp.stack([beta, (1.0 - beta) / width, 1.0 - beta, rate])

    smem = pl.BlockSpec(memory_space=pltpu.SMEM)

    def live(i, ints_ref):
        return jnp.minimum(i, ints_ref[1])

    new_rows, sums = pl.pallas_call(
        functools.partial(sums_kernel, group, mats, piece),
        grid_spec=pltpu.PrefetchScalarGridSpec(
            num_scalar_prefetch=1,
            grid=(steps,),
            in_specs=[
                smem,
                pl.BlockSpec((group, height, width), lambda i, s: (live(i, s), 0, 0)),
                pl.BlockSpec((group, height, 1), lambda i, s: (i, 0, 0)),
            ],
            out_specs=[
                pl.BlockSpec((group, height, 1), lambda i, s: (i, 0, 0)),
                pl.BlockSpec((8, width), lambda i, s: (0, 0)),
            ],
            scratch_shapes=[
                pltpu.VMEM((mats, 8, width), jnp.float32),
                pltpu.VMEM((mats, 8, width), jnp.float32),
                pltpu.VMEM((mats, 8, 128), jnp.float32),
            ],
        ),
        out_shape=[
            jax.ShapeDtypeStruct((slot_count, height, 1), jnp.float32),
            jax.ShapeDtypeStruct((8, width), jnp.float32),
        ],
        compiler_params=pltpu.CompilerParams(vmem_limit_bytes=60 * 2**20),
        cost_estimate=pl.CostEstimate(flops=grad.size * 6, bytes_accessed=grad.size * 4, transcendentals=0),
        name="sums",
    )(ints, floats, grad, row_state[:, :, None])

    pieces = sums.reshape(8, every, piece).transpose(1, 0, 2)
    pieces = lax.all_to_all(pieces, ("shard", "dp"), split_axis=0, concat_axis=0, tiled=True)
    total = lax.all_gather(jnp.sum(pieces, axis=0), ("shard", "dp"), axis=0)
    total = total.transpose(1, 0, 2).reshape(8, width)

    outs = pl.pallas_call(
        functools.partial(update_kernel, group, mats, parts, row_counts),
        grid_spec=pltpu.PrefetchScalarGridSpec(
            num_scalar_prefetch=1,
            grid=(steps,),
            in_specs=[
                smem,
                pl.BlockSpec((group, height, width), lambda i, s: (live(i, s), 0, 0)),
                pl.BlockSpec((group, height, width), lambda i, s: (live(i, s), 0, 0)),
                pl.BlockSpec((group, height, 1), lambda i, s: (live(i, s), 0, 0)),
                pl.BlockSpec((8, width), lambda i, s: (0, 0)),
                pl.BlockSpec((mats, width), lambda i, s: (0, 0)),
            ],
            out_specs=[
                pl.BlockSpec((parts, group, CHUNK, cut), lambda i, s: (0, live(i, s), 0, 0))
                for _ in range(chunks)
            ]
            + [pl.BlockSpec((mats, width), lambda i, s: (0, 0))],
            scratch_shapes=[pltpu.VMEM((mats, 1, width), jnp.float32)],
        ),
        out_shape=[
            jax.ShapeDtypeStruct((parts, slot_count, CHUNK, cut), jnp.bfloat16) for _ in range(chunks)
        ]
        + [jax.ShapeDtypeStruct((mats, width), jnp.float32)],
        compiler_params=pltpu.CompilerParams(vmem_limit_bytes=60 * 2**20),
        cost_estimate=pl.CostEstimate(flops=grad.size * 6, bytes_accessed=grad.size * 8, transcendentals=0),
        name="update",
    )(ints, floats, grad, param, new_rows, total, col_state)
    new_cols = outs[-1]

    dp = lax.axis_size("dp")
    piece_bytes = total_blocks * CHUNK * cut * 2
    placed = None
    run = 12 if total_blocks % 12 == 0 else 1
    for k in range(chunks):
        moved = lax.all_to_all(outs[k], "shard", split_axis=0, concat_axis=0, tiled=True)
        picked = pl.pallas_call(
            pick_kernel,
            in_specs=[smem, pl.BlockSpec(memory_space=pltpu.VMEM)],
            out_specs=pl.BlockSpec(memory_space=pltpu.VMEM),
            out_shape=jax.ShapeDtypeStruct((total_blocks, CHUNK, cut), jnp.bfloat16),
            compiler_params=pltpu.CompilerParams(vmem_limit_bytes=16 * 2**20),
            cost_estimate=pl.CostEstimate(flops=0, bytes_accessed=3 * piece_bytes, transcendentals=0),
            name="pick",
        )(slot_of, moved.reshape(parts * slot_count, CHUNK, cut))
        spread = lax.all_gather(picked, "dp", axis=1, tiled=True)
        spread = spread.reshape(total_blocks, dp, CHUNK, cut)
        old = [] if placed is None else [placed]
        placed = pl.pallas_call(
            place_kernel,
            grid=(total_blocks // run,),
            in_specs=[pl.BlockSpec((run, dp, CHUNK, cut), lambda i: (i, 0, 0, 0))]
            + [pl.BlockSpec(memory_space=pl.ANY) for _ in old],
            out_specs=pl.BlockSpec((run, dp, 1, CHUNK, cut), functools.partial(lambda k, i: (i, 0, k, 0, 0), k)),
            out_shape=jax.ShapeDtypeStruct((total_blocks, dp, chunks, CHUNK, cut), jnp.bfloat16),
            input_output_aliases={1: 0} if old else {},
            compiler_params=pltpu.CompilerParams(vmem_limit_bytes=60 * 2**20),
            cost_estimate=pl.CostEstimate(flops=0, bytes_accessed=2 * dp * piece_bytes, transcendentals=0),
            name="place",
        )(spread, *old)
    new_params = placed.reshape(total_blocks * dp * height, cut)
    return new_params, new_rows[:, :, 0], new_cols


def solution(mesh):
    return jax.shard_map(
        functools.partial(body, mesh.shape["shard"]),
        mesh=mesh,
        in_specs=(
            P("shard", "dp", None),
            P("shard", "dp", None),
            P("shard", "dp"),
            P(),
            P(),
            P(),
            P(),
        ),
        out_specs=(P(None, "shard"), P("shard", "dp"), P()),
        check_vma=False,
    )
```
